32 devices in a mesh: ep: 32 (over z, y, x, core).
Axes of the slice: x: 2, y: 2, z: 4, core: 2. Of those that a mesh axis runs over, the one named last changes fastest.
Arguments:
- hidden: bfloat16 [2, 1024, 3584], P(None, 'ep'), may hold values from -6 to 6
- expert_ids: int32 [2, 1024, 8], P(None, 'ep'), may hold values from 0 to 31, all different within a row; in each aligned block of 32 rows (0 to 31, 32 to 63, ..., all dimensions but the last counted through in order) at most 9 rows name the same one
- gate_scores: float32 [2, 1024, 8], P(None, 'ep'), may hold values from 0.05 to 1
- w_gate: bfloat16 [32, 3584, 1024], P('ep'), may hold values from -0.09375 to 0.09375
- w_up: bfloat16 [32, 3584, 1024], P('ep'), may hold values from -0.09375 to 0.09375
- w_down: bfloat16 [32, 1024, 3584], P('ep'), may hold values from -0.1875 to 0.1875
Outputs:
- mixed: bfloat16 [2, 1024, 3584], P(None, 'ep')
- expert_load: float32 [32], P('ep')
The draws below stay inside these ranges and needn't reach their ends.
Inputs may be any that keep to these rules, and one draw needn't show every extreme that they name: `expert_ids`: among the 32 rows of one device in one micro-batch, no expert is named by more than 9 rows, a bound that some block reaches. Each row names 8 different experts.
All inputs are finite; a program needn't handle non-finite values.
Results may differ from the reference program's by a relative error of at most 0.004.
The reference program's roundings to bfloat16 on the way (of `hid` and `answer`) count: a program that leaves them out, or rounds other values in their place, can miss the bound.
Values may be sent and summed in bfloat16 or wider, within the bound.
No kernel may reach another device: no remote copies, remote signals or barrier semaphores. Data moves between devices by JAX's collectives and lax.ppermute only.
A program may use at most 128 MiB of HBM per device.

```python
import math
import jax
import jax.numpy as jnp
import numpy as np
from jax import lax

D = 3584
FF = 1024
TOP = 8
MICRO = 2
TOK_MB = 32
EXPERTS = 32
TOKENS = 1024
CAP = 9
N_EP = 32


def levels(own_key, extent, split, least, largest):
    factor_of = 1.0
    for axis_at, shards_of in split:
        heights = jax.random.uniform(jax.random.fold_in(jax.random.fold_in(own_key, 6), axis_at), (shards_of,), jnp.float32, least / len(split), largest / len(split))
        factor_of = factor_of * jnp.repeat(jnp.exp(heights), extent[axis_at] // shards_of).reshape((-1,) + (1,) * (len(extent) - 1 - axis_at))
    return factor_of


def shared_out(key, own, number, rows, count, top, most, skew):
    order = jax.random.permutation(key, count)
    heavy_load, ordinary = load_shares(count, rows * top, most, skew, True), load_shares(count, rows * top, most, skew, False)
    places = jnp.arange(count)

    def named(lengths, turn):
        used = int((lengths > 0).sum())
        fixed = max(1, used // 4)
        moved = fixed + (places - fixed + turn * (used - fixed)) % max(1, count - fixed)
        return jnp.zeros((count,), jnp.int32).at[order[jnp.where(places < fixed, places, moved)]].set(jnp.asarray(lengths, jnp.int32))

    lengths = jnp.where(number % 4 == 0, named(heavy_load, number // 4), named(ordinary, number - number // 4 - 1))
    mixed = jax.random.permutation(jax.random.fold_in(own, 3), count)
    source_of, receiver = mixed[0:count // 2 * 2:2], mixed[1:count // 2 * 2:2]
    slack = jnp.minimum(lengths[source_of] - 1, most - lengths[receiver]) // 2
    slack = jnp.where((source_of == order[0]) | (receiver == order[0]) | (lengths[receiver] == 0), 0, jnp.maximum(slack, 0))
    moved = jax.random.randint(jax.random.fold_in(own, 4), (count // 2,), 0, 1 << 20) % (slack + 1)
    lengths = lengths.at[source_of].add(-moved).at[receiver].add(moved)
    members = jnp.searchsorted(jnp.cumsum(lengths), jnp.arange(rows * top), side="right").astype(jnp.int32)
    table = members.reshape(top, rows).T
    table = table[jax.random.permutation(jax.random.fold_in(own, 1), rows)]
    turn = jax.random.randint(jax.random.fold_in(own, 2), (rows, 1), 0, top)
    return jnp.take_along_axis(table, (jnp.arange(top)[None, :] + turn) % top, axis=1)


def load_shares(amount, total, limit, lean, full):
    loads = [(1 << 20) // math.isqrt(rank ** lean) + 1 for rank in range(1, amount + 1)]
    largest = limit if full else min(limit, max(-(-total // amount), total * loads[0] // sum(loads)))
    least = 1 if total - largest >= amount - 1 else 0
    holding, rest = [largest] + [least] * (amount - 1), total - largest - least * (amount - 1)
    while rest > 0:
        candidates = [i for i in range(1, amount) if holding[i] < largest] or [i for i in range(1, amount) if holding[i] < limit]
        mass, left = sum([loads[i] for i in candidates]), rest
        for i in candidates:
            extra = min(limit - holding[i], max(1, left * loads[i] // mass), rest)
            holding[i] = holding[i] + extra
            rest = rest - extra
    return np.array(holding)


def noise(stream_key, shape, deviation, bound, shards=(), kind=jnp.bfloat16):
    values = jax.random.normal(stream_key, shape, jnp.float32) * deviation
    if len(shards) > 0:
        values = levels(stream_key, shape, shards, -0.22, 0.18) * values
    return jnp.clip(values, min=-bound, max=bound).astype(kind)


def setup_inputs(seed: int = 0) -> dict:
    arg_keys = jax.random.split(jax.random.key(seed), 7)
    hidden = noise(arg_keys[0], (MICRO, TOKENS, D), 1.0, 6.0, ((1, 32),))
    expert_ids_keys = jax.random.split(jax.random.fold_in(arg_keys[1], 1), MICRO * TOKENS // TOK_MB)
    expert_ids_turns = jax.random.permutation(jax.random.fold_in(arg_keys[1], 3), MICRO * TOKENS // TOK_MB)
    expert_ids = jax.vmap(lambda own, number: shared_out(jax.random.fold_in(arg_keys[1], 2), own, number, TOK_MB, EXPERTS, TOP, CAP, 2))(expert_ids_keys, expert_ids_turns).reshape((MICRO, TOKENS, TOP))
    gate_scores = jnp.clip(jnp.exp(math.log(1.0) - 2.9957323 * jax.random.uniform(arg_keys[2], (MICRO, TOKENS, TOP), jnp.float32) ** levels(arg_keys[2], (MICRO, TOKENS, TOP), ((1, 32),), -0.2, 0.2)), 0.05, 1.0)
    w_gate = noise(arg_keys[3], (EXPERTS, D, FF), D ** -0.5, 0.09375, ((0, 32),))
    w_up = noise(arg_keys[4], (EXPERTS, D, FF), D ** -0.5, 0.09375, ((0, 32),))
    w_down = noise(arg_keys[5], (EXPERTS, FF, D), FF ** -0.5, 0.1875, ((0, 32),))
    return dict(hidden=hidden, expert_ids=expert_ids, gate_scores=gate_scores, w_gate=w_gate, w_up=w_up, w_down=w_down)


route_scale = 2.5


def reference(hidden, expert_ids, gate_scores, w_gate, w_up, w_down):
    weights = route_scale * gate_scores / jnp.sum(gate_scores, axis=-1, keepdims=True)
    grouped = expert_ids.reshape(MICRO, N_EP, TOK_MB * TOP)
    one_hot = (grouped[..., None] == jnp.arange(EXPERTS, dtype=jnp.int32)).astype(jnp.int32)
    earlier = jnp.cumsum(one_hot, axis=2) - one_hot
    slot_index = jnp.sum(earlier * one_hot, axis=-1).astype(jnp.int32)
    batch_axis = jnp.arange(MICRO, dtype=jnp.int32)[:, None, None]
    source_axis = jnp.arange(N_EP, dtype=jnp.int32)[None, :, None]
    owner = (jnp.arange(TOK_MB * TOP, dtype=jnp.int32) // TOP)[None, None, :]
    token_row = (owner + source_axis * TOK_MB + batch_axis * TOKENS).astype(jnp.int32)
    table = jnp.full((MICRO, EXPERTS, N_EP, CAP), MICRO * TOKENS, jnp.int32)
    table = table.at[batch_axis, grouped, source_axis, slot_index].set(token_row)
    shares = jnp.zeros((MICRO, EXPERTS, N_EP, CAP), jnp.float32)
    shares = shares.at[batch_axis, grouped, source_axis, slot_index].set(weights.reshape(MICRO, N_EP, TOK_MB * TOP))
    padded = jnp.concatenate([hidden.reshape(MICRO * TOKENS, D), jnp.zeros((1, D), jnp.bfloat16)], axis=0)

    def expert_step(total, expert):
        rows_index = table[:, expert].reshape(-1)
        gathered = padded[rows_index]
        gate = jnp.dot(gathered, w_gate[expert], preferred_element_type=jnp.float32)
        upper = jnp.dot(gathered, w_up[expert], preferred_element_type=jnp.float32)
        hid = (jax.nn.silu(gate) * upper).astype(jnp.bfloat16)
        answer = jnp.dot(hid, w_down[expert], preferred_element_type=jnp.float32).astype(jnp.bfloat16)
        scaled = shares[:, expert].reshape(-1)[:, None] * answer.astype(jnp.float32)
        return total.at[rows_index].add(scaled), None

    start = jnp.zeros((MICRO * TOKENS + 1, D), jnp.float32)
    total, unused = lax.scan(expert_step, start, jnp.arange(EXPERTS, dtype=jnp.int32))
    mixed = total[: MICRO * TOKENS].reshape(MICRO, TOKENS, D).astype(jnp.bfloat16)
    sums = jnp.zeros((EXPERTS,), jnp.float32).at[expert_ids.reshape(-1)].add(weights.reshape(-1))
    expert_load = sums * (EXPERTS / (route_scale * MICRO * TOKENS))
    return mixed, expert_load
```

```python
import functools
import jax
import jax.numpy as jnp
from jax import lax
from jax.experimental import pallas as pl
from jax.experimental.pallas import tpu as pltpu
from jax.sharding import PartitionSpec as P

route_scale = 2.5


def route(keys, shares, inner, tok_mb, capacity, rows):
    columns = keys.shape[1]
    hits = [keys == k for k in range(inner)]
    named = jnp.concatenate(
        [jnp.sum(jnp.where(hit, 1.0, 0.0), axis=0, keepdims=True) for hit in hits], axis=0
    )
    share = [jnp.sum(jnp.where(hit, shares, 0.0), axis=0, keepdims=True) for hit in hits]
    before = lax.broadcasted_iota(jnp.int32, (columns, columns), 0)
    after = lax.broadcasted_iota(jnp.int32, (columns, columns), 1)
    lower = (before < after) & (before // tok_mb == after // tok_mb)
    slot = jnp.dot(
        named.astype(jnp.bfloat16),
        jnp.where(lower, 1.0, 0.0).astype(jnp.bfloat16),
        preferred_element_type=jnp.float32,
    )
    source = lax.broadcasted_iota(jnp.int32, (inner, columns), 1) // tok_mb
    target = jnp.where(named > 0.5, source * capacity + slot.astype(jnp.int32), -1)
    row = lax.broadcasted_iota(jnp.int32, (rows, columns), 0)
    chosen = [row == target[k : k + 1] for k in range(inner)]
    return chosen, share


def pack_kernel(outer, inner, tok_mb, capacity, rows, *refs):
    keys_ref, shares_ref = refs[:2]
    blocks = refs[2 : 2 + outer]
    outs = refs[2 + outer : 2 + outer + inner]
    sel_ref = refs[-1]

    @pl.when(pl.program_id(0) == 0)
    def _():
        chosen, _ = route(keys_ref[...], shares_ref[...], inner, tok_mb, capacity, rows)
        for k in range(inner):
            sel_ref[k * rows : (k + 1) * rows] = jnp.where(chosen[k], 1.0, 0.0).astype(jnp.bfloat16)

    tokens = jnp.concatenate([block[...] for block in blocks], axis=0)
    picked = jnp.dot(sel_ref[...], tokens, preferred_element_type=jnp.float32).astype(jnp.bfloat16)
    for k in range(inner):
        outs[k][...] = picked[k * rows : (k + 1) * rows]


def expert_kernel(inner, rows, *refs):
    blocks = refs[:inner]
    gate_ref, up_ref, down_ref = refs[inner : inner + 3]
    outs = refs[inner + 3 : 2 * inner + 3]
    joined, total = refs[2 * inner + 3 :]
    step = pl.program_id(0)

    @pl.when(step == 0)
    def _():
        for k in range(inner):
            joined[k * rows : (k + 1) * rows] = blocks[k][...]

    tokens = joined[...]
    gate = jnp.dot(tokens, gate_ref[0], preferred_element_type=jnp.float32)
    upper = jnp.dot(tokens, up_ref[0], preferred_element_type=jnp.float32)
    hid = (gate / (1.0 + jnp.exp(-gate)) * upper).astype(jnp.bfloat16)
    term = jnp.dot(hid, down_ref[0], preferred_element_type=jnp.float32)

    @pl.when(step == 0)
    def _():
        total[...] = term

    @pl.when(step > 0)
    def _():
        total[...] += term

    @pl.when(step == pl.num_programs(0) - 1)
    def _():
        for k in range(inner):
            outs[k][...] = total[k * rows : (k + 1) * rows].astype(jnp.bfloat16)


def combine_kernel(outer, inner, tok_mb, capacity, rows, *refs):
    keys_ref, shares_ref = refs[:2]
    blocks = refs[2 : 2 + inner]
    outs = refs[2 + inner : 2 + inner + outer]
    parts_ref = refs[-1]

    @pl.when(pl.program_id(0) == 0)
    def _():
        chosen, share = route(keys_ref[...], shares_ref[...], inner, tok_mb, capacity, rows)
        for k in range(inner):
            rest = jnp.where(chosen[k], share[k], 0.0)
            for part in range(3):
                piece = rest.astype(jnp.bfloat16)
                parts_ref[part, k * rows : (k + 1) * rows] = piece
                rest = rest - piece.astype(jnp.float32)

    answers = jnp.concatenate([block[...] for block in blocks], axis=0)
    summed = None
    for part in (2, 1, 0):
        term = lax.dot_general(
            parts_ref[part], answers, (((0,), (0,)), ((), ())), preferred_element_type=jnp.float32
        )
        summed = term if summed is None else summed + term
    for k in range(outer):
        outs[k][...] = summed[k * tok_mb : (k + 1) * tok_mb].astype(outs[k].dtype)


def pieces(width, most):
    step = width
    while step > most and step % 256 == 0:
        step //= 2
    return step


def shards(hidden, expert_ids, gate_scores, w_gate, w_up, w_down):
    devices = lax.axis_size("ep")
    me = lax.axis_index("ep")
    micro_count, tok_mb, width = hidden.shape
    chosen = expert_ids.shape[2]
    experts = devices * w_gate.shape[0]
    hidden_units = w_gate.shape[2]
    assert w_gate.shape[0] == 1 and devices & (devices - 1) == 0
    capacity = tok_mb * chosen // experts + 1
    inner = 1
    while inner * inner < devices:
        inner *= 2
    outer = devices // inner
    rows = -(-outer * capacity // 8) * 8
    columns = outer * tok_mb

    def outer_swap(value, k):
        return lax.ppermute(value, "ep", [(d, d ^ (k * inner)) for d in range(devices)])

    def inner_swap(value, k):
        return lax.ppermute(value, "ep", [(d, d ^ k) for d in range(devices)])

    weights = route_scale * gate_scores / jnp.sum(gate_scores, axis=-1, keepdims=True)
    meta = jnp.concatenate([expert_ids.astype(jnp.float32), weights], axis=2).transpose(0, 2, 1)
    metas = [meta] + [outer_swap(meta, k) for k in range(1, outer)]
    spread = [
        [hidden[b]] + [outer_swap(hidden[b], k) for k in range(1, outer)]
        for b in range(micro_count)
    ]
    meta = jnp.concatenate(metas, axis=2)
    keys = meta[:, :chosen].astype(jnp.int32) ^ me
    shares = meta[:, chosen:]

    lane = pieces(width, 1024)
    steps = width // lane
    small = pl.BlockSpec((chosen, columns), lambda i: (0, 0))
    token_spec = pl.BlockSpec((tok_mb, lane), lambda i: (0, i))
    row_spec = pl.BlockSpec((rows, lane), lambda i: (0, i))
    row_shape = jax.ShapeDtypeStruct((rows, width), jnp.bfloat16)
    whole = pl.BlockSpec((rows, width), lambda i: (0, 0))
    few = pieces(hidden_units, 256)
    sizes = (outer, inner, tok_mb, capacity, rows)

    def pack(b):
        return pl.pallas_call(
            functools.partial(pack_kernel, *sizes),
            grid=(steps,),
            in_specs=[small, small] + [token_spec] * outer,
            out_specs=[row_spec] * inner,
            out_shape=[row_shape] * inner,
            scratch_shapes=[pltpu.VMEM((inner * rows, columns), jnp.bfloat16)],
            cost_estimate=pl.CostEstimate(
                flops=2 * inner * rows * columns * width,
                bytes_accessed=2 * (inner * rows + columns) * width,
                transcendentals=0,
            ),
            name="pack",
        )(keys[b], shares[b], *spread[b])

    def expert(blocks):
        return pl.pallas_call(
            functools.partial(expert_kernel, inner, rows),
            grid=(hidden_units // few,),
            in_specs=[whole] * inner
            + [
                pl.BlockSpec((1, width, few), lambda i: (0, 0, i)),
                pl.BlockSpec((1, width, few), lambda i: (0, 0, i)),
                pl.BlockSpec((1, few, width), lambda i: (0, i, 0)),
            ],
            out_specs=[whole] * inner,
            out_shape=[row_shape] * inner,
            scratch_shapes=[
                pltpu.VMEM((inner * rows, width), jnp.bfloat16),
                pltpu.VMEM((inner * rows, width), jnp.float32),
            ],
            compiler_params=pltpu.CompilerParams(vmem_limit_bytes=48 * 1024 * 1024),
            cost_estimate=pl.CostEstimate(
                flops=6 * inner * rows * width * hidden_units,
                bytes_accessed=6 * width * hidden_units + 4 * inner * rows * width,
                transcendentals=inner * rows * hidden_units,
            ),
            name="expert",
        )(*blocks, w_gate, w_up, w_down)

    def combine(b, blocks):
        return pl.pallas_call(
            functools.partial(combine_kernel, *sizes),
            grid=(steps,),
            in_specs=[small, small] + [row_spec] * inner,
            out_specs=[token_spec] * outer,
            out_shape=[
                jax.ShapeDtypeStruct((tok_mb, width), jnp.float32 if k == 0 else jnp.bfloat16)
                for k in range(outer)
            ],
            scratch_shapes=[pltpu.VMEM((3, inner * rows, columns), jnp.bfloat16)],
            cost_estimate=pl.CostEstimate(
                flops=6 * inner * rows * columns * width,
                bytes_accessed=2 * (inner * rows + columns) * width,
                transcendentals=0,
            ),
            name="combine",
        )(keys[b], shares[b], *blocks)

    def exchange(blocks, swap):
        return [blocks[0]] + [swap(blocks[k], k) for k in range(1, len(blocks))]

    arrived = [exchange(pack(b), inner_swap) for b in range(micro_count)]
    answered = [exchange(expert(arrived[b]), inner_swap) for b in range(micro_count)]
    results = []
    for b in range(micro_count):
        parts = exchange(combine(b, answered[b]), outer_swap)
        total = parts[0]
        for part in parts[1:]:
            total = total + part.astype(jnp.float32)
        results.append(total.astype(jnp.bfloat16))
    mixed = jnp.stack(results, axis=0)

    all_ids = expert_ids.reshape(-1)
    one_hot = (all_ids[:, None] == jnp.arange(experts, dtype=jnp.int32)[None, :]).astype(
        jnp.float32
    )
    local_term = jnp.sum(one_hot * weights.reshape(-1)[:, None], axis=0)
    summed_load = lax.psum_scatter(local_term, "ep", scatter_dimension=0, tiled=True)
    expert_load = summed_load * (experts / (route_scale * micro_count * tok_mb * devices))
    return (mixed, expert_load)


def solution(mesh):
    placed = (
        P(None, "ep", None),
        P(None, "ep", None),
        P(None, "ep", None),
        P("ep", None, None),
        P("ep", None, None),
        P("ep", None, None),
    )
    return jax.shard_map(
        shards,
        mesh=mesh,
        in_specs=placed,
        out_specs=(P(None, "ep", None), P("ep")),
        check_vma=False,
    )
```

```python
import functools
import jax
import jax.numpy as jnp
from jax import lax
from jax.experimental import pallas as pl
from jax.experimental.pallas import tpu as pltpu
from jax.sharding import PartitionSpec as P

route_scale = 2.5


def route(keys, shares, inner, tok_mb, capacity, rows):
    columns = keys.shape[1]
    hits = [keys == k for k in range(inner)]
    named = jnp.concatenate(
        [jnp.sum(jnp.where(hit, 1.0, 0.0), axis=0, keepdims=True) for hit in hits], axis=0
    )
    share = [jnp.sum(jnp.where(hit, shares, 0.0), axis=0, keepdims=True) for hit in hits]
    before = lax.broadcasted_iota(jnp.int32, (columns, columns), 0)
    after = lax.broadcasted_iota(jnp.int32, (columns, columns), 1)
    lower = (before < after) & (before // tok_mb == after // tok_mb)
    slot = jnp.dot(
        named.astype(jnp.bfloat16),
        jnp.where(lower, 1.0, 0.0).astype(jnp.bfloat16),
        preferred_element_type=jnp.float32,
    )
    source = lax.broadcasted_iota(jnp.int32, (inner, columns), 1) // tok_mb
    target = jnp.where(named > 0.5, source * capacity + slot.astype(jnp.int32), -1)
    row = lax.broadcasted_iota(jnp.int32, (rows, columns), 0)
    chosen = [row == target[k : k + 1] for k in range(inner)]
    return chosen, share


def pack_kernel(outer, inner, tok_mb, capacity, rows, *refs):
    keys_ref, shares_ref = refs[:2]
    blocks = refs[2 : 2 + outer]
    outs = refs[2 + outer : 2 + outer + inner]
    sel_ref = refs[-1]

    @pl.when(pl.program_id(0) == 0)
    def _():
        chosen, _ = route(keys_ref[...], shares_ref[...], inner, tok_mb, capacity, rows)
        for k in range(inner):
            sel_ref[k * rows : (k + 1) * rows] = jnp.where(chosen[k], 1.0, 0.0).astype(jnp.bfloat16)

    tokens = jnp.concatenate([block[...] for block in blocks], axis=0)
    picked = jnp.dot(sel_ref[...], tokens, preferred_element_type=jnp.float32).astype(jnp.bfloat16)
    for k in range(inner):
        outs[k][...] = picked[k * rows : (k + 1) * rows]


def expert_kernel(inner, rows, *refs):
    blocks = refs[:inner]
    gate_ref, up_ref, down_ref = refs[inner : inner + 3]
    outs = refs[inner + 3 : 2 * inner + 3]
    joined, total = refs[2 * inner + 3 :]
    step = pl.program_id(0)

    @pl.when(step == 0)
    def _():
        for k in range(inner):
            joined[k * rows : (k + 1) * rows] = blocks[k][...]

    tokens = joined[...]
    gate = jnp.dot(tokens, gate_ref[0], preferred_element_type=jnp.float32)
    upper = jnp.dot(tokens, up_ref[0], preferred_element_type=jnp.float32)
    hid = (gate / (1.0 + jnp.exp(-gate)) * upper).astype(jnp.bfloat16)
    term = jnp.dot(hid, down_ref[0], preferred_element_type=jnp.float32)

    @pl.when(step == 0)
    def _():
        total[...] = term

    @pl.when(step > 0)
    def _():
        total[...] += term

    @pl.when(step == pl.num_programs(0) - 1)
    def _():
        for k in range(inner):
            outs[k][...] = total[k * rows : (k + 1) * rows].astype(jnp.bfloat16)


def combine_kernel(outer, inner, tok_mb, capacity, rows, *refs):
    keys_ref, shares_ref = refs[:2]
    blocks = refs[2 : 2 + inner]
    outs = refs[2 + inner : 2 + inner + outer]
    parts_ref = refs[-1]

    @pl.when(pl.program_id(0) == 0)
    def _():
        chosen, share = route(keys_ref[...], shares_ref[...], inner, tok_mb, capacity, rows)
        for k in range(inner):
            rest = jnp.where(chosen[k], share[k], 0.0)
            for part in range(3):
                piece = rest.astype(jnp.bfloat16)
                parts_ref[part, k * rows : (k + 1) * rows] = piece
                rest = rest - piece.astype(jnp.float32)

    answers = jnp.concatenate([block[...] for block in blocks], axis=0)
    summed = None
    for part in (2, 1, 0):
        term = lax.dot_general(
            parts_ref[part], answers, (((0,), (0,)), ((), ())), preferred_element_type=jnp.float32
        )
        summed = term if summed is None else summed + term
    for k in range(outer):
        outs[k][...] = summed[k * tok_mb : (k + 1) * tok_mb].astype(outs[k].dtype)


def pieces(width, most):
    step = width
    while step > most and step % 256 == 0:
        step //= 2
    return step


def shards(hidden, expert_ids, gate_scores, w_gate, w_up, w_down):
    devices = lax.axis_size("ep")
    me = lax.axis_index("ep")
    micro_count, tok_mb, width = hidden.shape
    chosen = expert_ids.shape[2]
    experts = devices * w_gate.shape[0]
    hidden_units = w_gate.shape[2]
    assert w_gate.shape[0] == 1 and devices & (devices - 1) == 0
    capacity = tok_mb * chosen // experts + 1
    inner = 1
    while inner * inner < devices:
        inner *= 2
    outer = devices // inner
    rows = -(-outer * capacity // 8) * 8
    columns = outer * tok_mb

    def outer_swap(value, k):
        return lax.ppermute(value, "ep", [(d, d ^ (k * inner)) for d in range(devices)])

    def inner_swap(value, k):
        return lax.ppermute(value, "ep", [(d, d ^ k) for d in range(devices)])

    weights = route_scale * gate_scores / jnp.sum(gate_scores, axis=-1, keepdims=True)
    meta = jnp.concatenate([expert_ids.astype(jnp.float32), weights], axis=2).transpose(0, 2, 1)
    metas = [meta] + [outer_swap(meta, k) for k in range(1, outer)]
    spread = []
    for b in range(micro_count):
        spread.append([hidden[b]] + [outer_swap(hidden[b], k) for k in range(1, outer)])
    meta = jnp.concatenate(metas, axis=2)
    keys = meta[:, :chosen].astype(jnp.int32) ^ me
    shares = meta[:, chosen:]

    partners = jnp.arange(inner, dtype=jnp.int32)[:, None, None, None]
    load = jnp.sum(jnp.where(keys[None] == partners, shares[None], 0.0), axis=(1, 2, 3))
    half = inner // 2
    while half:
        load = load[:half] + inner_swap(load[half:], half)
        half //= 2
    keys, load = lax.optimization_barrier((keys, load))
    expert_load = load * (experts / (route_scale * micro_count * tok_mb * devices))

    lane = pieces(width, 1024)
    steps = width // lane
    small = pl.BlockSpec((chosen, columns), lambda i: (0, 0))
    token_spec = pl.BlockSpec((tok_mb, lane), lambda i: (0, i))
    row_spec = pl.BlockSpec((rows, lane), lambda i: (0, i))
    row_shape = jax.ShapeDtypeStruct((rows, width), jnp.bfloat16)
    whole = pl.BlockSpec((rows, width), lambda i: (0, 0))
    few = pieces(hidden_units, 256)
    sizes = (outer, inner, tok_mb, capacity, rows)

    def pack(b):
        return pl.pallas_call(
            functools.partial(pack_kernel, *sizes),
            grid=(steps,),
            in_specs=[small, small] + [token_spec] * outer,
            out_specs=[row_spec] * inner,
            out_shape=[row_shape] * inner,
            scratch_shapes=[pltpu.VMEM((inner * rows, columns), jnp.bfloat16)],
            cost_estimate=pl.CostEstimate(
                flops=2 * inner * rows * columns * width,
                bytes_accessed=2 * (inner * rows + columns) * width,
                transcendentals=0,
            ),
            name="pack",
        )(keys[b], shares[b], *spread[b])

    def expert(blocks):
        return pl.pallas_call(
            functools.partial(expert_kernel, inner, rows),
            grid=(hidden_units // few,),
            in_specs=[whole] * inner
            + [
                pl.BlockSpec((1, width, few), lambda i: (0, 0, i)),
                pl.BlockSpec((1, width, few), lambda i: (0, 0, i)),
                pl.BlockSpec((1, few, width), lambda i: (0, i, 0)),
            ],
            out_specs=[whole] * inner,
            out_shape=[row_shape] * inner,
            scratch_shapes=[
                pltpu.VMEM((inner * rows, width), jnp.bfloat16),
                pltpu.VMEM((inner * rows, width), jnp.float32),
            ],
            compiler_params=pltpu.CompilerParams(vmem_limit_bytes=48 * 1024 * 1024),
            cost_estimate=pl.CostEstimate(
                flops=6 * inner * rows * width * hidden_units,
                bytes_accessed=6 * width * hidden_units + 4 * inner * rows * width,
                transcendentals=inner * rows * hidden_units,
            ),
            name="expert",
        )(*blocks, w_gate, w_up, w_down)

    def combine(b, blocks):
        return pl.pallas_call(
            functools.partial(combine_kernel, *sizes),
            grid=(steps,),
            in_specs=[small, small] + [row_spec] * inner,
            out_specs=[token_spec] * outer,
            out_shape=[
                jax.ShapeDtypeStruct((tok_mb, width), jnp.float32 if k == 0 else jnp.bfloat16)
                for k in range(outer)
            ],
            scratch_shapes=[pltpu.VMEM((3, inner * rows, columns), jnp.bfloat16)],
            cost_estimate=pl.CostEstimate(
                flops=6 * inner * rows * columns * width,
                bytes_accessed=2 * (inner * rows + columns) * width,
                transcendentals=0,
            ),
            name="combine",
        )(keys[b], shares[b], *blocks)

    def exchange(blocks, swap):
        return [blocks[0]] + [swap(blocks[k], k) for k in range(1, len(blocks))]

    arrived = [exchange(pack(b), inner_swap) for b in range(micro_count)]
    answered = [exchange(expert(arrived[b]), inner_swap) for b in range(micro_count)]
    results = []
    for b in range(micro_count):
        parts = exchange(combine(b, answered[b]), outer_swap)
        total = parts[0]
        for part in parts[1:]:
            total = total + part.astype(jnp.float32)
        results.append(total.astype(jnp.bfloat16))
    mixed = jnp.stack(results, axis=0)
    return (mixed, expert_load)


def solution(mesh):
    placed = (
        P(None, "ep", None),
        P(None, "ep", None),
        P(None, "ep", None),
        P("ep", None, None),
        P("ep", None, None),
        P("ep", None, None),
    )

    return jax.shard_map(
        shards,
        mesh=mesh,
        in_specs=placed,
        out_specs=(P(None, "ep", None), P("ep")),
        check_vma=False,
    )
```
